16 devices in a mesh: mat: 2 (over y, z), dp: 8 (over x, core).
Axes of the slice: x: 4, y: 2, z: 1, core: 2. Of those that a mesh axis runs over, the one named last changes fastest.
The devices are a block of a 4x4x8 slice.
Arguments:
- a_mat: bfloat16 [9216, 65536], P('mat', 'dp'), parts along dimension 0
Outputs:
- output: float32 [16, 5, 576, 576], P(('mat', 'dp')), parts along dimension 0
There are 2 independent parts. The reference program is written for one: setup_inputs(seed, part) draws one part's arguments, and reference() takes and returns one part's arrays. A program takes and returns all parts, laid end to end along the dimension named above; each array names one.
All inputs are finite; a program needn't handle non-finite values.
Results may differ from the reference program's by a relative error of at most 0.001.
Values are sent between devices in bfloat16 or wider.
A program may use at most 768 MiB of HBM per device.

```python
import jax
import jax.numpy as jnp
from jax import lax

GRAM_ORDER = 4608
COLS_DEV = 8192
GROUPS = 8
MIX_RANK = 8

BLOCK = GRAM_ORDER // GROUPS
SLOTS = GROUPS // 2 + 1
WIDTH = COLS_DEV * GROUPS


def pair_table():
    half = GROUPS // 2
    hi_list = []
    lo_list = []
    for dev_index in range(GROUPS):
        for slot in range(SLOTS):
            other_id = (dev_index - slot) % GROUPS
            if slot < half or dev_index < half:
                hi_list.append(max(dev_index, other_id))
                lo_list.append(min(dev_index, other_id))
            else:
                hi_list.append(-1)
                lo_list.append(-1)
    return jnp.array(hi_list, dtype=jnp.int32), jnp.array(lo_list, dtype=jnp.int32)


def setup_inputs(seed: int = 0, part: int = 0) -> dict:
    key = jax.random.fold_in(jax.random.key(seed), part)
    key_mix, key_src, key_gain = jax.random.split(key, 3)
    mixers = jax.random.normal(key_mix, (GROUPS, GRAM_ORDER, MIX_RANK), jnp.float32) * MIX_RANK ** -0.5
    sources = jax.random.normal(key_src, (GROUPS, MIX_RANK, COLS_DEV), jnp.float32)
    block_gain = jax.random.uniform(key_gain, (GROUPS,), jnp.float32, minval=0.7, maxval=1.4)
    row_gain = jnp.repeat(block_gain, BLOCK)
    mixed = jnp.einsum('snr,srk->nsk', mixers, sources).reshape(GRAM_ORDER, WIDTH)
    scale = (MIX_RANK ** 0.5 / (COLS_DEV * GROUPS ** 0.5)) ** 0.5
    a_mat = mixed * (row_gain[:, None] * scale)
    return {'a_mat': a_mat.astype(jnp.bfloat16)}


def reference(a_mat):
    hi_ids, lo_ids = pair_table()

    def one_block(pair_ids):
        hi_id, lo_id = pair_ids
        hi_rows = lax.dynamic_slice_in_dim(a_mat, jnp.maximum(hi_id, 0) * BLOCK, BLOCK, axis=0)
        lo_rows = lax.dynamic_slice_in_dim(a_mat, jnp.maximum(lo_id, 0) * BLOCK, BLOCK, axis=0)
        block_prod = jnp.dot(hi_rows, lo_rows.T, preferred_element_type=jnp.float32)
        return jnp.where(hi_id >= 0, block_prod, 0.0)

    blocks = lax.map(one_block, (hi_ids, lo_ids))
    return blocks.reshape(GROUPS, SLOTS, BLOCK, BLOCK)
```

```python
import functools

import jax
import jax.numpy as jnp
from jax import lax
from jax.experimental import pallas as pl
from jax.experimental.pallas import tpu as pltpu
from jax.sharding import PartitionSpec as P

MAIN = 512
DLAND = 3
RING = 14


def select(index, values):
    out = jnp.int32(values[-1])
    for k in range(len(values) - 2, -1, -1):
        out = jnp.where(index == k, jnp.int32(values[k]), out)
    return out


def kernel(groups, a_ref, out_ref, land, lhs, rhs, res, dland, sbuf, srem, rbuf, remf, fin,
           lhs_sem, rhs_sem, dsend, drecv, credit, ssend, rsend, lrecv, load_sem, fin_sem):
    chips = groups // 2
    half = groups // 2
    rows = lhs.shape[1]
    hrows = rows // 2
    rest = rows - MAIN
    visits = groups
    far = visits - 2
    strips = half + 2
    total = visits + groups * (half + 1) - half
    me = lax.axis_index('dp')
    x, c = me // 2, me % 2
    partner = x * 2 + (1 - c)

    def dest(v):
        off = select(v, (2, 2, 1, chips - 1, 1, chips - 1, 0, 0))
        core = select(v, (0, 1, 0, 0, 1, 1, 0, 1))
        chip = (x + off) % chips
        return chip * 2 + core, core

    def slots_of(p):
        return jnp.where(p < half, half + 1, half)

    def via_plus(p, s):
        mains = select(p, (2, 2, 3, 4, 3, 2, 1, 2))
        return jnp.where(s == 0, select(p, (0, 1, 0, 0, 0, 1, 0, 0)) == 1, s - 1 < mains)

    def widths(p, s):
        wide = p < half
        return (
            (MAIN, s > 0),
            (384, jnp.logical_and(s == 0, wide)),
            (256, jnp.logical_and(s == 0, jnp.logical_not(wide))),
        )

    def on_route(v, p, s):
        plus = via_plus(p, s)
        right = jnp.logical_or(v == 2, v == 4)
        there = jnp.where(right, jnp.logical_not(plus), plus)
        return jnp.logical_and(jnp.logical_and(v >= 2, v < far), there)

    def first_slot(side, core, s):
        return (side * 2 + core) * strips + s

    def last_slot(side, part, s):
        return (4 + side * 2 + part) * strips + s

    def start_lhs(v):
        p, _ = dest(v)
        pltpu.make_async_copy(
            a_ref.at[pl.ds(pl.multiple_of(p * rows, 64), rows)], lhs.at[v % 2], lhs_sem.at[v % 2]
        ).start()

    def start_rhs(v, s, slot):
        p, _ = dest(v)

        @pl.when(s > 0)
        def _():
            q = (p - (s - 1) + groups) % groups
            pltpu.make_async_copy(
                a_ref.at[pl.ds(pl.multiple_of(q * rows, 64), MAIN)], rhs.at[slot], rhs_sem.at[slot]
            ).start()

        def piece(t, k):
            q = (p - t + groups) % groups
            pltpu.make_async_copy(
                a_ref.at[pl.ds(pl.multiple_of(q * rows + MAIN, 64), rest)],
                rhs.at[slot, pl.ds(k * rest, rest)],
                rhs_sem.at[slot],
            ).start()

        @pl.when(s == 0)
        def _():
            for t in range(half):
                piece(t, t)

            @pl.when(p < half)
            def _():
                piece(half, half)
                piece(0, half + 1)

    def signal_credit(kr, received):
        @pl.when(kr + DLAND < received)
        def _():
            pl.semaphore_signal(credit.at[kr % DLAND], inc=1, device_id={'dp': partner}, device_id_type=pl.DeviceIdType.MESH)

    own = me
    received = total - (slots_of(own) + 1)

    def before(v, s):
        p, core = dest(v)
        for width, cond in widths(p, s):
            @pl.when(jnp.logical_and(cond, on_route(v, p, s)))
            def _():
                side = jnp.where(jnp.logical_or(v == 2, v == 4), 0, 1)
                k = first_slot(side, core, s)
                block = land.at[k, :, pl.ds(0, width)]
                pltpu.make_async_copy(block, block, lrecv.at[k]).wait()
                pltpu.make_async_copy(block, rbuf.at[0, pl.ds(0, hrows), pl.ds(0, width)], load_sem.at[0]).start()

            @pl.when(jnp.logical_and(cond, jnp.logical_and(v >= far, core == c)))
            def _():
                for side in range(2):
                    for part in range(2):
                        k = last_slot(side, part, s)
                        block = land.at[k, :, pl.ds(0, width)]
                        pltpu.make_async_copy(block, block, lrecv.at[k]).wait()
                        pltpu.make_async_copy(
                            block,
                            rbuf.at[side, pl.ds(part * hrows, hrows), pl.ds(0, width)],
                            load_sem.at[side * 2 + part],
                        ).start()

    def after(v, s, slot, kt, kr):
        p, core = dest(v)
        k = kr % DLAND
        mine = pl.ds(pl.multiple_of(c * hrows, 8), hrows)
        other = pl.ds(pl.multiple_of((1 - c) * hrows, 8), hrows)
        plus = via_plus(p, s)
        right = jnp.logical_or(v == 2, v == 4)
        routed = on_route(v, p, s)
        hop = jnp.where(plus, (x + chips - 1) % chips, (x + 1) % chips)
        target = jnp.where(v < 2, hop * 2 + c, p)
        place = jnp.where(
            v < 2,
            first_slot(jnp.where(plus, 1, 0), core, s),
            last_slot(jnp.where(right, 0, 1), c, s),
        )

        for width, cond in widths(p, s):
            cols = pl.ds(0, width)

            @pl.when(jnp.logical_and(cond, v < far))
            def _():
                got = dland.at[k, pl.ds(0, hrows), cols]
                pltpu.make_async_copy(got, got, drecv.at[k]).wait()

                def send(buf, sem):
                    val = res[slot, mine, cols] + dland[k, pl.ds(0, hrows), cols]

                    @pl.when(routed)
                    def _():
                        add = rbuf.at[0, pl.ds(0, hrows), cols]
                        pltpu.make_async_copy(add, add, load_sem.at[0]).wait()
                        buf[...] = res[slot, mine, cols] + dland[k, pl.ds(0, hrows), cols] + rbuf[0, pl.ds(0, hrows), cols]

                    @pl.when(jnp.logical_not(routed))
                    def _():
                        buf[...] = res[slot, mine, cols] + dland[k, pl.ds(0, hrows), cols]

                    pltpu.make_async_remote_copy(
                        src_ref=buf,
                        dst_ref=land.at[place, :, cols],
                        send_sem=sem,
                        recv_sem=lrecv.at[place],
                        device_id={'dp': target},
                        device_id_type=pl.DeviceIdType.MESH,
                    ).start()

                if width == MAIN:
                    ring = kt % RING

                    @pl.when(kt >= RING)
                    def _():
                        pltpu.make_async_copy(sbuf.at[ring], sbuf.at[ring], ssend.at[ring]).wait()

                    send(sbuf.at[ring], ssend.at[ring])
                else:
                    send(srem.at[v, :, cols], rsend.at[v])
                sent = res.at[slot, other, cols]
                pltpu.make_async_copy(sent, sent, dsend.at[slot]).wait()
                signal_credit(kr, received)

            @pl.when(jnp.logical_and(cond, jnp.logical_and(v >= far, core == c)))
            def _():
                got = dland.at[k, :, cols]
                pltpu.make_async_copy(got, got, drecv.at[k]).wait()
                for side in range(2):
                    for part in range(2):
                        add = rbuf.at[side, pl.ds(part * hrows, hrows), cols]
                        pltpu.make_async_copy(add, add, load_sem.at[side * 2 + part]).wait()

                def whole():
                    return res[slot, :, cols] + dland[k, :, cols] + (rbuf[0, :, cols] + rbuf[1, :, cols])

                if width != MAIN:
                    remf[:, cols] = whole()
                else:
                    t = s - 1

                    @pl.when(t > 0)
                    def _():
                        pltpu.make_async_copy(fin, fin, fin_sem).wait()

                    @pl.when(t <= p)
                    def _():
                        fin[:, cols] = whole()
                        for i in range(half + 1):
                            @pl.when(t == i)
                            def _():
                                fin[:, pl.ds(MAIN, rest)] = remf[:, pl.ds(i * rest, rest)]

                    @pl.when(t > p)
                    def _():
                        fin[pl.ds(0, MAIN), :] = whole().T
                        for i in range(half + 1):
                            @pl.when(t == i)
                            def _():
                                pair = remf[:, pl.ds(i // 2 * 128, 128)].T
                                fin[pl.ds(MAIN, rest), :] = pair[i % 2 * rest:(i % 2 + 1) * rest]

                    pltpu.make_async_copy(fin, out_ref.at[t], fin_sem).start()
                signal_credit(kr, received)

            @pl.when(jnp.logical_and(cond, jnp.logical_and(v >= far, core != c)))
            def _():
                sent = res.at[slot, :, cols]
                pltpu.make_async_copy(sent, sent, dsend.at[slot]).wait()

        takes = jnp.logical_or(v < far, core == c)
        kr = kr + jnp.where(takes, 1, 0)
        kt = kt + jnp.where(jnp.logical_and(v < far, s > 0), 1, 0)
        return kt, kr

    start_lhs(jnp.int32(0))
    start_rhs(jnp.int32(0), jnp.int32(0), 0)

    barrier = pltpu.get_barrier_semaphore()
    peers = [partner]
    for step in (1, chips - 1):
        for core in range(2):
            peers.append((x + step) % chips * 2 + core)
    for peer in peers:
        pl.semaphore_signal(barrier, inc=1, device_id={'dp': peer}, device_id_type=pl.DeviceIdType.MESH)
    pl.semaphore_wait(barrier, len(peers))

    @pl.when(own >= half)
    def _():
        fin[...] = jnp.zeros_like(fin)
        pad = pltpu.make_async_copy(fin, out_ref.at[half], fin_sem)
        pad.start()
        pad.wait()

    def step(g, carry):
        v, s, pv, ps, kt, ks, kr = carry
        p, core = dest(v)
        slot = g % 2
        nt = slots_of(p)
        end = s == nt
        nv = jnp.where(end, v + 1, v)
        ns = jnp.where(end, 0, s + 1)

        for width, cond in widths(p, s):
            @pl.when(cond)
            def _():
                block = rhs.at[slot, pl.ds(0, width)]
                pltpu.make_async_copy(block, block, rhs_sem.at[slot]).wait()

        @pl.when(g + 1 < total)
        def _():
            start_rhs(nv, ns, 1 - slot)

        @pl.when(s == 0)
        def _():
            pltpu.make_async_copy(lhs.at[v % 2], lhs.at[v % 2], lhs_sem.at[v % 2]).wait()

            @pl.when(v + 1 < visits)
            def _():
                start_lhs(v + 1)

        @pl.when(g > 0)
        def _():
            before(pv, ps)

        for width, cond in widths(p, s):
            @pl.when(cond)
            def _():
                res[slot, :, pl.ds(0, width)] = lax.dot_general(
                    lhs[v % 2], rhs[slot, pl.ds(0, width)], (((1,), (1,)), ((), ())),
                    preferred_element_type=jnp.float32,
                )

        gives = jnp.logical_or(v < far, core != c)
        k = ks % DLAND

        @pl.when(jnp.logical_and(gives, ks >= DLAND))
        def _():
            pl.semaphore_wait(credit.at[k], 1)

        for width, cond in widths(p, s):
            cols = pl.ds(0, width)

            def give(src_rows, dst_rows):
                pltpu.make_async_remote_copy(
                    src_ref=res.at[slot, src_rows, cols],
                    dst_ref=dland.at[k, dst_rows, cols],
                    send_sem=dsend.at[slot],
                    recv_sem=drecv.at[k],
                    device_id={'dp': partner},
                    device_id_type=pl.DeviceIdType.MESH,
                ).start()

            @pl.when(jnp.logical_and(cond, v < far))
            def _():
                give(pl.ds(pl.multiple_of((1 - c) * hrows, 8), hrows), pl.ds(0, hrows))

            @pl.when(jnp.logical_and(cond, jnp.logical_and(v >= far, core != c)))
            def _():
                give(pl.ds(0, rows), pl.ds(0, rows))

        ks = ks + jnp.where(gives, 1, 0)

        @pl.when(g > 0)
        def _():
            after(pv, ps, 1 - slot, kt, kr)

        takes = jnp.logical_and(g > 0, jnp.logical_or(pv < far, dest(pv)[1] == c))
        kr = kr + jnp.where(takes, 1, 0)
        kt = kt + jnp.where(jnp.logical_and(g > 0, jnp.logical_and(pv < far, ps > 0)), 1, 0)
        return nv, ns, v, s, kt, ks, kr

    zero = jnp.int32(0)
    _, _, pv, ps, kt, ks, kr = lax.fori_loop(0, total, step, (zero,) * 7)
    before(pv, ps)
    after(pv, ps, (total - 1) % 2, kt, kr)

    for ring in range(RING):
        pltpu.make_async_copy(sbuf.at[ring], sbuf.at[ring], ssend.at[ring]).wait()
    for v in range(far):
        p, _ = dest(jnp.int32(v))
        for width, cond in widths(p, jnp.int32(0))[1:]:
            @pl.when(cond)
            def _():
                block = srem.at[v, :, pl.ds(0, width)]
                pltpu.make_async_copy(block, block, rsend.at[v]).wait()
    pltpu.make_async_copy(fin, fin, fin_sem).wait()


def solution(mesh):
    groups = mesh.shape['dp']

    def local_gram(a_local):
        n_rows, cols = a_local.shape
        rows = n_rows // groups
        hrows = rows // 2
        slots = groups // 2 + 1
        landing = 8 * (slots + 1)
        out, _ = pl.pallas_call(
            functools.partial(kernel, groups),
            out_shape=(
                jax.ShapeDtypeStruct((slots, rows, rows), jnp.float32),
                jax.ShapeDtypeStruct((landing, hrows, MAIN), jnp.float32),
            ),
            in_specs=[pl.BlockSpec(memory_space=pl.ANY)],
            out_specs=(pl.BlockSpec(memory_space=pl.ANY), pl.BlockSpec(memory_space=pl.ANY)),
            scratch_shapes=[
                pltpu.VMEM((2, rows, cols), jnp.bfloat16),
                pltpu.VMEM((2, MAIN, cols), jnp.bfloat16),
                pltpu.VMEM((2, rows, MAIN), jnp.float32),
                pltpu.VMEM((DLAND, rows, MAIN), jnp.float32),
                pltpu.VMEM((RING, hrows, MAIN), jnp.float32),
                pltpu.VMEM((groups - 2, hrows, 384), jnp.float32),
                pltpu.VMEM((2, rows, MAIN), jnp.float32),
                pltpu.VMEM((rows, 384), jnp.float32),
                pltpu.VMEM((rows, rows), jnp.float32),
                pltpu.SemaphoreType.DMA((2,)),
                pltpu.SemaphoreType.DMA((2,)),
                pltpu.SemaphoreType.DMA((2,)),
                pltpu.SemaphoreType.DMA((DLAND,)),
                pltpu.SemaphoreType.REGULAR((DLAND,)),
                pltpu.SemaphoreType.DMA((RING,)),
                pltpu.SemaphoreType.DMA((groups - 2,)),
                pltpu.SemaphoreType.DMA((landing,)),
                pltpu.SemaphoreType.DMA((4,)),
                pltpu.SemaphoreType.DMA,
            ],
            compiler_params=pltpu.CompilerParams(
                collective_id=0, has_side_effects=True, vmem_limit_bytes=67_000_000
            ),
            name='gram_reduce',
        )(a_local)
        return out.reshape(slots, rows, rows)[None]

    return jax.shard_map(local_gram, mesh=mesh, in_specs=(P('mat', 'dp'),), out_specs=P(('mat', 'dp')), check_vma=False)
```

```python
import functools

import jax
import jax.numpy as jnp
from jax import lax
from jax.experimental import pallas as pl
from jax.experimental.pallas import tpu as pltpu
from jax.sharding import PartitionSpec as P

MAIN = 512
DLAND = 3
RING = 14


def select(index, values):
    out = jnp.int32(values[-1])
    for k in range(len(values) - 2, -1, -1):
        out = jnp.where(index == k, jnp.int32(values[k]), out)
    return out


def kernel(groups, a_ref, out_ref, land, lhs, rhs, res, dland, sbuf, srem, rbuf, remf, fin,
           lhs_sem, rhs_sem, dsend, drecv, credit, ssend, rsend, lrecv, load_sem, fin_sem):
    chips = groups // 2
    half = groups // 2
    rows = lhs.shape[1]
    hrows = rows // 2
    rest = rows - MAIN
    visits = groups
    far = visits - 2
    strips = half + 2
    total = visits + groups * (half + 1) - half
    me = lax.axis_index('dp')
    x, c = me // 2, me % 2
    partner = x * 2 + (1 - c)

    def rightward(v):
        return (v % 2 == 0) == ((x + 1) % chips >= chips // 2)

    def dest(v):
        side = jnp.where(rightward(v), 1, chips - 1)
        off = jnp.where(v < 2, 2, jnp.where(v < far, side, 0))
        core = select(v, (0, 1, 0, 0, 1, 1, 0, 1))
        chip = (x + off) % chips
        return chip * 2 + core, core

    def slots_of(p):
        return jnp.where(p < half, half + 1, half)

    def via_plus(p, s):
        masks = select(p, (0b010100, 0b010101, 0b101010, 0b110110, 0b010110, 0b001011, 0b000100, 0b010100))
        return masks // select(s, (1, 2, 4, 8, 16, 32)) % 2 == 1

    def strip_at(v, i):
        return jnp.where(v < far, jnp.where(i == slots_of(dest(v)[0]), 0, i + 1), i)

    def following(v, s):
        nt = slots_of(dest(v)[0])
        paired = jnp.logical_and(v >= 2, v < far)
        first = v % 2 == 0
        mate = jnp.where(first, v + 1, v - 1)
        mate_s = jnp.where(first, s, s + 1)
        take_mate = jnp.logical_and(paired, mate_s <= slots_of(dest(mate)[0]))
        more = s < nt
        later = jnp.where(jnp.logical_and(paired, first), v + 2, v + 1)
        nv = jnp.where(take_mate, mate, jnp.where(more, v, later))
        ns = jnp.where(take_mate, mate_s, jnp.where(more, s + 1, 0))
        return nv, ns

    def widths(p, s):
        wide = p < half
        return (
            (MAIN, s > 0),
            (384, jnp.logical_and(s == 0, wide)),
            (256, jnp.logical_and(s == 0, jnp.logical_not(wide))),
        )

    def on_route(v, p, s):
        plus = via_plus(p, s)
        right = rightward(v)
        there = jnp.where(right, jnp.logical_not(plus), plus)
        return jnp.logical_and(jnp.logical_and(v >= 2, v < far), there)

    def first_slot(side, core, s):
        return (side * 2 + core) * strips + s

    def last_slot(side, part, s):
        return (4 + side * 2 + part) * strips + s

    def start_lhs(v):
        p, _ = dest(v)
        pltpu.make_async_copy(
            a_ref.at[pl.ds(pl.multiple_of(p * rows, 64), rows)], lhs.at[v % 2], lhs_sem.at[v % 2]
        ).start()

    def start_rhs(v, s, slot):
        p, _ = dest(v)

        @pl.when(s > 0)
        def _():
            q = (p - (s - 1) + groups) % groups
            pltpu.make_async_copy(
                a_ref.at[pl.ds(pl.multiple_of(q * rows, 64), MAIN)], rhs.at[slot], rhs_sem.at[slot]
            ).start()

        def piece(t, k):
            q = (p - t + groups) % groups
            pltpu.make_async_copy(
                a_ref.at[pl.ds(pl.multiple_of(q * rows + MAIN, 64), rest)],
                rhs.at[slot, pl.ds(k * rest, rest)],
                rhs_sem.at[slot],
            ).start()

        @pl.when(s == 0)
        def _():
            for t in range(half):
                piece(t, t)

            @pl.when(p < half)
            def _():
                piece(half, half)
                piece(0, half + 1)

    def signal_credit(kr, received):
        @pl.when(kr + DLAND < received)
        def _():
            pl.semaphore_signal(credit.at[kr % DLAND], inc=1, device_id={'dp': partner}, device_id_type=pl.DeviceIdType.MESH)

    own = me
    received = total - (slots_of(own) + 1)

    def before(v, s):
        p, core = dest(v)
        for width, cond in widths(p, s):
            @pl.when(jnp.logical_and(cond, on_route(v, p, s)))
            def _():
                side = jnp.where(rightward(v), 0, 1)
                k = first_slot(side, core, s)
                block = land.at[k, :, pl.ds(0, width)]
                pltpu.make_async_copy(block, block, lrecv.at[k]).wait()
                pltpu.make_async_copy(block, rbuf.at[0, pl.ds(0, hrows), pl.ds(0, width)], load_sem.at[0]).start()

            @pl.when(jnp.logical_and(cond, jnp.logical_and(v >= far, core == c)))
            def _():
                for side in range(2):
                    for part in range(2):
                        k = last_slot(side, part, s)
                        block = land.at[k, :, pl.ds(0, width)]
                        pltpu.make_async_copy(block, block, lrecv.at[k]).wait()
                        pltpu.make_async_copy(
                            block,
                            rbuf.at[side, pl.ds(part * hrows, hrows), pl.ds(0, width)],
                            load_sem.at[side * 2 + part],
                        ).start()

    def after(v, s, slot, kt, kr):
        p, core = dest(v)
        k = kr % DLAND
        mine = pl.ds(pl.multiple_of(c * hrows, 8), hrows)
        other = pl.ds(pl.multiple_of((1 - c) * hrows, 8), hrows)
        plus = via_plus(p, s)
        right = rightward(v)
        routed = on_route(v, p, s)
        hop = jnp.where(plus, (x + chips - 1) % chips, (x + 1) % chips)
        target = jnp.where(v < 2, hop * 2 + c, p)
        place = jnp.where(
            v < 2,
            first_slot(jnp.where(plus, 1, 0), core, s),
            last_slot(jnp.where(right, 0, 1), c, s),
        )

        for width, cond in widths(p, s):
            cols = pl.ds(0, width)

            @pl.when(jnp.logical_and(cond, v < far))
            def _():
                got = dland.at[k, pl.ds(0, hrows), cols]
                pltpu.make_async_copy(got, got, drecv.at[k]).wait()

                def send(buf, sem):
                    val = res[slot, mine, cols] + dland[k, pl.ds(0, hrows), cols]

                    @pl.when(routed)
                    def _():
                        add = rbuf.at[0, pl.ds(0, hrows), cols]
                        pltpu.make_async_copy(add, add, load_sem.at[0]).wait()
                        buf[...] = res[slot, mine, cols] + dland[k, pl.ds(0, hrows), cols] + rbuf[0, pl.ds(0, hrows), cols]

                    @pl.when(jnp.logical_not(routed))
                    def _():
                        buf[...] = res[slot, mine, cols] + dland[k, pl.ds(0, hrows), cols]

                    pltpu.make_async_remote_copy(
                        src_ref=buf,
                        dst_ref=land.at[place, :, cols],
                        send_sem=sem,
                        recv_sem=lrecv.at[place],
                        device_id={'dp': target},
                        device_id_type=pl.DeviceIdType.MESH,
                    ).start()

                if width == MAIN:
                    ring = kt % RING

                    @pl.when(kt >= RING)
                    def _():
                        pltpu.make_async_copy(sbuf.at[ring], sbuf.at[ring], ssend.at[ring]).wait()

                    send(sbuf.at[ring], ssend.at[ring])
                else:
                    send(srem.at[v, :, cols], rsend.at[v])
                sent = res.at[slot, other, cols]
                pltpu.make_async_copy(sent, sent, dsend.at[slot]).wait()
                signal_credit(kr, received)

            @pl.when(jnp.logical_and(cond, jnp.logical_and(v >= far, core == c)))
            def _():
                got = dland.at[k, :, cols]
                pltpu.make_async_copy(got, got, drecv.at[k]).wait()
                for side in range(2):
                    for part in range(2):
                        add = rbuf.at[side, pl.ds(part * hrows, hrows), cols]
                        pltpu.make_async_copy(add, add, load_sem.at[side * 2 + part]).wait()

                def whole():
                    return res[slot, :, cols] + dland[k, :, cols] + (rbuf[0, :, cols] + rbuf[1, :, cols])

                if width != MAIN:
                    remf[:, cols] = whole()
                else:
                    t = s - 1

                    @pl.when(t > 0)
                    def _():
                        pltpu.make_async_copy(fin, fin, fin_sem).wait()

                    @pl.when(t <= p)
                    def _():
                        fin[:, cols] = whole()
                        for i in range(half + 1):
                            @pl.when(t == i)
                            def _():
                                fin[:, pl.ds(MAIN, rest)] = remf[:, pl.ds(i * rest, rest)]

                    @pl.when(t > p)
                    def _():
                        fin[pl.ds(0, MAIN), :] = whole().T
                        for i in range(half + 1):
                            @pl.when(t == i)
                            def _():
                                pair = remf[:, pl.ds(i // 2 * 128, 128)].T
                                fin[pl.ds(MAIN, rest), :] = pair[i % 2 * rest:(i % 2 + 1) * rest]

                    pltpu.make_async_copy(fin, out_ref.at[t], fin_sem).start()
                signal_credit(kr, received)

            @pl.when(jnp.logical_and(cond, jnp.logical_and(v >= far, core != c)))
            def _():
                sent = res.at[slot, :, cols]
                pltpu.make_async_copy(sent, sent, dsend.at[slot]).wait()

        takes = jnp.logical_or(v < far, core == c)
        kr = kr + jnp.where(takes, 1, 0)
        kt = kt + jnp.where(jnp.logical_and(v < far, s > 0), 1, 0)
        return kt, kr

    start_lhs(jnp.int32(0))
    start_rhs(jnp.int32(0), jnp.int32(1), 0)

    barrier = pltpu.get_barrier_semaphore()
    peers = [partner]
    for step in (1, chips - 1):
        for core in range(2):
            peers.append((x + step) % chips * 2 + core)
    for peer in peers:
        pl.semaphore_signal(barrier, inc=1, device_id={'dp': peer}, device_id_type=pl.DeviceIdType.MESH)
    pl.semaphore_wait(barrier, len(peers))

    @pl.when(own >= half)
    def _():
        fin[...] = jnp.zeros_like(fin)
        pad = pltpu.make_async_copy(fin, out_ref.at[half], fin_sem)
        pad.start()
        pad.wait()

    def step(g, carry):
        v, i, pv, pi, kt, ks, kr = carry
        p, core = dest(v)
        s, ps = strip_at(v, i), strip_at(pv, pi)
        slot = g % 2
        nv, ni = following(v, i)

        for width, cond in widths(p, s):
            @pl.when(cond)
            def _():
                block = rhs.at[slot, pl.ds(0, width)]
                pltpu.make_async_copy(block, block, rhs_sem.at[slot]).wait()

        @pl.when(g + 1 < total)
        def _():
            start_rhs(nv, strip_at(nv, ni), 1 - slot)

        @pl.when(g == 1)
        def _():
            start_lhs(jnp.int32(1))

        @pl.when(jnp.logical_and(g > 0, jnp.logical_and(pi == slots_of(dest(pv)[0]), pv + 2 < visits)))
        def _():
            start_lhs(pv + 2)

        @pl.when(i == 0)
        def _():
            pltpu.make_async_copy(lhs.at[v % 2], lhs.at[v % 2], lhs_sem.at[v % 2]).wait()

        @pl.when(g > 0)
        def _():
            before(pv, ps)

        for width, cond in widths(p, s):
            @pl.when(cond)
            def _():
                res[slot, :, pl.ds(0, width)] = lax.dot_general(
                    lhs[v % 2], rhs[slot, pl.ds(0, width)], (((1,), (1,)), ((), ())),
                    preferred_element_type=jnp.float32,
                )

        gives = jnp.logical_or(v < far, core != c)
        k = ks % DLAND

        @pl.when(jnp.logical_and(gives, ks >= DLAND))
        def _():
            pl.semaphore_wait(credit.at[k], 1)

        for width, cond in widths(p, s):
            cols = pl.ds(0, width)

            def give(src_rows, dst_rows):
                pltpu.make_async_remote_copy(
                    src_ref=res.at[slot, src_rows, cols],
                    dst_ref=dland.at[k, dst_rows, cols],
                    send_sem=dsend.at[slot],
                    recv_sem=drecv.at[k],
                    device_id={'dp': partner},
                    device_id_type=pl.DeviceIdType.MESH,
                ).start()

            @pl.when(jnp.logical_and(cond, v < far))
            def _():
                give(pl.ds(pl.multiple_of((1 - c) * hrows, 8), hrows), pl.ds(0, hrows))

            @pl.when(jnp.logical_and(cond, jnp.logical_and(v >= far, core != c)))
            def _():
                give(pl.ds(0, rows), pl.ds(0, rows))

        ks = ks + jnp.where(gives, 1, 0)

        @pl.when(g > 0)
        def _():
            after(pv, ps, 1 - slot, kt, kr)

        takes = jnp.logical_and(g > 0, jnp.logical_or(pv < far, dest(pv)[1] == c))
        kr = kr + jnp.where(takes, 1, 0)
        kt = kt + jnp.where(jnp.logical_and(g > 0, jnp.logical_and(pv < far, ps > 0)), 1, 0)
        return nv, ni, v, i, kt, ks, kr

    zero = jnp.int32(0)
    _, _, pv, pi, kt, ks, kr = lax.fori_loop(0, total, step, (zero,) * 7)
    ps = strip_at(pv, pi)
    before(pv, ps)
    after(pv, ps, (total - 1) % 2, kt, kr)

    for ring in range(RING):
        pltpu.make_async_copy(sbuf.at[ring], sbuf.at[ring], ssend.at[ring]).wait()
    for v in range(far):
        p, _ = dest(jnp.int32(v))
        for width, cond in widths(p, jnp.int32(0))[1:]:
            @pl.when(cond)
            def _():
                block = srem.at[v, :, pl.ds(0, width)]
                pltpu.make_async_copy(block, block, rsend.at[v]).wait()
    pltpu.make_async_copy(fin, fin, fin_sem).wait()


def solution(mesh):
    groups = mesh.shape['dp']

    def local_gram(a_local):
        n_rows, cols = a_local.shape
        rows = n_rows // groups
        hrows = rows // 2
        slots = groups // 2 + 1
        landing = 8 * (slots + 1)
        out, _ = pl.pallas_call(
            functools.partial(kernel, groups),
            out_shape=(
                jax.ShapeDtypeStruct((slots, rows, rows), jnp.float32),
                jax.ShapeDtypeStruct((landing, hrows, MAIN), jnp.float32),
            ),
            in_specs=[pl.BlockSpec(memory_space=pl.ANY)],
            out_specs=(pl.BlockSpec(memory_space=pl.ANY), pl.BlockSpec(memory_space=pl.ANY)),
            scratch_shapes=[
                pltpu.VMEM((2, rows, cols), jnp.bfloat16),
                pltpu.VMEM((2, MAIN, cols), jnp.bfloat16),
                pltpu.VMEM((2, rows, MAIN), jnp.float32),
                pltpu.VMEM((DLAND, rows, MAIN), jnp.float32),
                pltpu.VMEM((RING, hrows, MAIN), jnp.float32),
                pltpu.VMEM((groups - 2, hrows, 384), jnp.float32),
                pltpu.VMEM((2, rows, MAIN), jnp.float32),
                pltpu.VMEM((rows, 384), jnp.float32),
                pltpu.VMEM((rows, rows), jnp.float32),
                pltpu.SemaphoreType.DMA((2,)),
                pltpu.SemaphoreType.DMA((2,)),
                pltpu.SemaphoreType.DMA((2,)),
                pltpu.SemaphoreType.DMA((DLAND,)),
                pltpu.SemaphoreType.REGULAR((DLAND,)),
                pltpu.SemaphoreType.DMA((RING,)),
                pltpu.SemaphoreType.DMA((groups - 2,)),
                pltpu.SemaphoreType.DMA((landing,)),
                pltpu.SemaphoreType.DMA((4,)),
                pltpu.SemaphoreType.DMA,
            ],
            compiler_params=pltpu.CompilerParams(
                collective_id=0, has_side_effects=True, vmem_limit_bytes=67_000_000
            ),
            name='gram_reduce',
        )(a_local)
        return out.reshape(slots, rows, rows)[None]

    return jax.shard_map(local_gram, mesh=mesh, in_specs=(P('mat', 'dp'),), out_specs=P(('mat', 'dp')), check_vma=False)
```

```python
import functools

import jax
import jax.numpy as jnp
from jax import lax
from jax.experimental import pallas as pl
from jax.experimental.pallas import tpu as pltpu
from jax.sharding import PartitionSpec as P

MAIN = 512
DLAND = 3
RING = 14


def select(index, values):
    out = jnp.int32(values[-1])
    for k in range(len(values) - 2, -1, -1):
        out = jnp.where(index == k, jnp.int32(values[k]), out)
    return out


def kernel(groups, a_ref, out_ref, land, lhs, rhs, res, dland, sbuf, srem, rbuf, remf, fin,
           lhs_sem, rhs_sem, dsend, drecv, credit, ssend, rsend, lrecv, load_sem, fin_sem):
    chips = groups // 2
    half = groups // 2
    rows = lhs.shape[1]
    hrows = rows // 2
    rest = rows - MAIN
    visits = groups
    far = visits - 2
    strips = half + 2
    total = visits + groups * (half + 1) - half
    me = lax.axis_index('dp')
    x, c = lax.div(me, 2), lax.rem(me, 2)
    partner = x * 2 + (1 - c)

    upper_right = lax.rem(x + 1, chips) >= chips // 2

    def rightward(v):
        return (lax.rem(v, 2) == 0) == upper_right

    def dest(v):
        side = jnp.where(rightward(v), 1, chips - 1)
        off = jnp.where(v < 2, 2, jnp.where(v < far, side, 0))
        core = jnp.where(jnp.logical_or(jnp.logical_or(v == 1, v == 7), jnp.logical_or(v == 4, v == 5)), 1, 0)
        chip = lax.rem(x + off, chips)
        return chip * 2 + core, core

    def slots_of(p):
        return jnp.where(p < half, half + 1, half)

    def via_plus(p, s):
        masks = select(p, (0b010100, 0b010101, 0b101010, 0b110110, 0b010110, 0b001011, 0b000100, 0b010100))
        return lax.rem(lax.div(masks, select(s, (1, 2, 4, 8, 16, 32))), 2) == 1

    def strip_at(v, i):
        swapped = jnp.where(i < 2, 1 - i, i)
        return jnp.where(v < 2, jnp.where(i == slots_of(dest(v)[0]), 0, i + 1), jnp.where(v < far, swapped, i))

    def following(v, s):
        nt = slots_of(dest(v)[0])
        paired = jnp.logical_and(v >= 2, v < far)
        first = lax.rem(v, 2) == 0
        mate = jnp.where(first, v + 1, v - 1)
        mate_s = jnp.where(first, s, s + 1)
        take_mate = jnp.logical_and(paired, mate_s <= slots_of(dest(mate)[0]))
        more = s < nt
        later = jnp.where(jnp.logical_and(paired, first), v + 2, v + 1)
        nv = jnp.where(take_mate, mate, jnp.where(more, v, later))
        ns = jnp.where(take_mate, mate_s, jnp.where(more, s + 1, 0))
        return nv, ns

    def widths(p, s):
        wide = p < half
        return (
            (MAIN, s > 0),
            (384, jnp.logical_and(s == 0, wide)),
            (256, jnp.logical_and(s == 0, jnp.logical_not(wide))),
        )

    def on_route(v, p, s):
        plus = via_plus(p, s)
        right = rightward(v)
        there = jnp.where(right, jnp.logical_not(plus), plus)
        return jnp.logical_and(jnp.logical_and(v >= 2, v < far), there)

    def first_slot(side, core, s):
        return (side * 2 + core) * strips + s

    def last_slot(side, part, s):
        return (4 + side * 2 + part) * strips + s

    def start_lhs(v):
        p, _ = dest(v)
        pltpu.make_async_copy(
            a_ref.at[pl.ds(pl.multiple_of(p * rows, 64), rows)], lhs.at[lax.rem(v, 2)], lhs_sem.at[lax.rem(v, 2)]
        ).start()

    def start_rhs(v, s, slot):
        p, _ = dest(v)

        @pl.when(s > 0)
        def _():
            q = lax.rem(p - (s - 1) + groups, groups)
            pltpu.make_async_copy(
                a_ref.at[pl.ds(pl.multiple_of(q * rows, 64), MAIN)], rhs.at[slot], rhs_sem.at[slot]
            ).start()

        def piece(t, k):
            q = lax.rem(p - t + groups, groups)
            pltpu.make_async_copy(
                a_ref.at[pl.ds(pl.multiple_of(q * rows + MAIN, 64), rest)],
                rhs.at[slot, pl.ds(k * rest, rest)],
                rhs_sem.at[slot],
            ).start()

        @pl.when(s == 0)
        def _():
            for t in range(half):
                piece(t, t)

            @pl.when(p < half)
            def _():
                piece(half, half)
                piece(0, half + 1)

    def signal_credit(kr, received):
        @pl.when(kr + DLAND < received)
        def _():
            pl.semaphore_signal(credit.at[lax.rem(kr, DLAND)], inc=1, device_id={'dp': partner}, device_id_type=pl.DeviceIdType.MESH)

    own = me
    received = total - (slots_of(own) + 1)

    def before(v, s):
        p, core = dest(v)
        for width, cond in widths(p, s):
            @pl.when(jnp.logical_and(cond, on_route(v, p, s)))
            def _():
                side = jnp.where(rightward(v), 0, 1)
                k = first_slot(side, core, s)
                block = land.at[k, :, pl.ds(0, width)]
                pltpu.make_async_copy(block, block, lrecv.at[k]).wait()
                pltpu.make_async_copy(block, rbuf.at[0, pl.ds(0, hrows), pl.ds(0, width)], load_sem.at[0]).start()

            @pl.when(jnp.logical_and(cond, jnp.logical_and(v >= far, core == c)))
            def _():
                for side in range(2):
                    for part in range(2):
                        k = last_slot(side, part, s)
                        block = land.at[k, :, pl.ds(0, width)]
                        pltpu.make_async_copy(block, block, lrecv.at[k]).wait()
                        pltpu.make_async_copy(
                            block,
                            rbuf.at[side, pl.ds(part * hrows, hrows), pl.ds(0, width)],
                            load_sem.at[side * 2 + part],
                        ).start()

    def after(v, s, slot, kt, kr):
        p, core = dest(v)
        k = lax.rem(kr, DLAND)
        mine = pl.ds(pl.multiple_of(c * hrows, 8), hrows)
        other = pl.ds(pl.multiple_of((1 - c) * hrows, 8), hrows)
        plus = via_plus(p, s)
        right = rightward(v)
        routed = on_route(v, p, s)
        hop = lax.rem(x + jnp.where(plus, chips - 1, 1), chips)
        target = jnp.where(v < 2, hop * 2 + c, p)
        place = jnp.where(
            v < 2,
            first_slot(jnp.where(plus, 1, 0), core, s),
            last_slot(jnp.where(right, 0, 1), c, s),
        )

        for width, cond in widths(p, s):
            cols = pl.ds(0, width)

            @pl.when(jnp.logical_and(cond, v < far))
            def _():
                got = dland.at[k, pl.ds(0, hrows), cols]
                pltpu.make_async_copy(got, got, drecv.at[k]).wait()

                def send(buf, sem):
                    val = res[slot, mine, cols] + dland[k, pl.ds(0, hrows), cols]

                    @pl.when(routed)
                    def _():
                        add = rbuf.at[0, pl.ds(0, hrows), cols]
                        pltpu.make_async_copy(add, add, load_sem.at[0]).wait()
                        buf[...] = res[slot, mine, cols] + dland[k, pl.ds(0, hrows), cols] + rbuf[0, pl.ds(0, hrows), cols]

                    @pl.when(jnp.logical_not(routed))
                    def _():
                        buf[...] = res[slot, mine, cols] + dland[k, pl.ds(0, hrows), cols]

                    pltpu.make_async_remote_copy(
                        src_ref=buf,
                        dst_ref=land.at[place, :, cols],
                        send_sem=sem,
                        recv_sem=lrecv.at[place],
                        device_id={'dp': target},
                        device_id_type=pl.DeviceIdType.MESH,
                    ).start()

                if width == MAIN:
                    ring = lax.rem(kt, RING)

                    @pl.when(kt >= RING)
                    def _():
                        pltpu.make_async_copy(sbuf.at[ring], sbuf.at[ring], ssend.at[ring]).wait()

                    send(sbuf.at[ring], ssend.at[ring])
                else:
                    send(srem.at[v, :, cols], rsend.at[v])
                sent = res.at[slot, other, cols]
                pltpu.make_async_copy(sent, sent, dsend.at[slot]).wait()
                signal_credit(kr, received)

            @pl.when(jnp.logical_and(cond, jnp.logical_and(v >= far, core == c)))
            def _():
                got = dland.at[k, :, cols]
                pltpu.make_async_copy(got, got, drecv.at[k]).wait()
                for side in range(2):
                    for part in range(2):
                        add = rbuf.at[side, pl.ds(part * hrows, hrows), cols]
                        pltpu.make_async_copy(add, add, load_sem.at[side * 2 + part]).wait()

                def whole():
                    return res[slot, :, cols] + dland[k, :, cols] + (rbuf[0, :, cols] + rbuf[1, :, cols])

                if width != MAIN:
                    remf[:, cols] = whole()
                else:
                    t = s - 1

                    @pl.when(t > 0)
                    def _():
                        pltpu.make_async_copy(fin, fin, fin_sem).wait()

                    @pl.when(t == 0)
                    def _():
                        def part(top, bottom, left, right):
                            at = (slice(top, bottom), slice(left, right))
                            return res[(slot, *at)] + dland[(k, *at)] + (rbuf[(0, *at)] + rbuf[(1, *at)])

                        lower = part(256, rows, 0, 256)
                        fin[0:256, 0:256] = part(0, 256, 0, 256)
                        fin[256:rows, 0:256] = lower
                        fin[0:256, 256:MAIN] = lower[0:256].T
                        fin[256:rows, 256:MAIN] = part(256, rows, 256, MAIN)
                        fin[:, pl.ds(MAIN, rest)] = remf[:, pl.ds(0, rest)]

                    @pl.when(jnp.logical_and(t > 0, t <= p))
                    def _():
                        fin[:, cols] = whole()
                        for i in range(1, half + 1):
                            @pl.when(t == i)
                            def _():
                                fin[:, pl.ds(MAIN, rest)] = remf[:, pl.ds(i * rest, rest)]

                    @pl.when(t > p)
                    def _():
                        fin[pl.ds(0, MAIN), :] = whole().T
                        for i in range(1, half + 1):
                            @pl.when(t == i)
                            def _():
                                pair = remf[:, pl.ds(i // 2 * 128, 128)].T
                                fin[pl.ds(MAIN, rest), :] = pair[i % 2 * rest:(i % 2 + 1) * rest]

                    pltpu.make_async_copy(fin, out_ref.at[t], fin_sem).start()
                signal_credit(kr, received)

            @pl.when(jnp.logical_and(cond, jnp.logical_and(v >= far, core != c)))
            def _():
                sent = res.at[slot, :, cols]
                pltpu.make_async_copy(sent, sent, dsend.at[slot]).wait()

        takes = jnp.logical_or(v < far, core == c)
        kr = kr + jnp.where(takes, 1, 0)
        kt = kt + jnp.where(jnp.logical_and(v < far, s > 0), 1, 0)
        return kt, kr

    start_lhs(jnp.int32(0))
    start_rhs(jnp.int32(0), jnp.int32(1), 0)

    barrier = pltpu.get_barrier_semaphore()
    peers = [partner]
    for step in (1, chips - 1):
        for core in range(2):
            peers.append((x + step) % chips * 2 + core)
    for peer in peers:
        pl.semaphore_signal(barrier, inc=1, device_id={'dp': peer}, device_id_type=pl.DeviceIdType.MESH)
    pl.semaphore_wait(barrier, len(peers))

    @pl.when(own >= half)
    def _():
        fin[...] = jnp.zeros_like(fin)
        pad = pltpu.make_async_copy(fin, out_ref.at[half], fin_sem)
        pad.start()
        pad.wait()

    def step(g, carry):
        v, i, pv, pi, kt, ks, kr = carry
        p, core = dest(v)
        s, ps = strip_at(v, i), strip_at(pv, pi)
        slot = lax.rem(g, 2)
        nv, ni = following(v, i)

        for width, cond in widths(p, s):
            @pl.when(cond)
            def _():
                block = rhs.at[slot, pl.ds(0, width)]
                pltpu.make_async_copy(block, block, rhs_sem.at[slot]).wait()

        @pl.when(g + 1 < total)
        def _():
            start_rhs(nv, strip_at(nv, ni), 1 - slot)

        @pl.when(g == 1)
        def _():
            start_lhs(jnp.int32(1))

        @pl.when(jnp.logical_and(g > 0, jnp.logical_and(pi == slots_of(dest(pv)[0]), pv + 2 < visits)))
        def _():
            start_lhs(pv + 2)

        held = lax.rem(v, 2)

        @pl.when(i == 0)
        def _():
            pltpu.make_async_copy(lhs.at[held], lhs.at[held], lhs_sem.at[held]).wait()

        @pl.when(g > 0)
        def _():
            before(pv, ps)

        def product(width, top=0, left=0):
            res[slot, top:rows, left:width] = lax.dot_general(
                lhs[held, top:rows], rhs[slot, left:width], (((1,), (1,)), ((), ())), preferred_element_type=jnp.float32
            )

        @pl.when(s > 1)
        def _():
            product(MAIN)

        @pl.when(s == 1)
        def _():
            product(256)
            product(MAIN, 256, 256)

        for width, cond in widths(p, s)[1:]:
            @pl.when(cond)
            def _():
                product(width)

        gives = jnp.logical_or(v < far, core != c)
        k = lax.rem(ks, DLAND)

        @pl.when(jnp.logical_and(gives, ks >= DLAND))
        def _():
            pl.semaphore_wait(credit.at[k], 1)

        for width, cond in widths(p, s):
            cols = pl.ds(0, width)

            def give(src_rows, dst_rows):
                pltpu.make_async_remote_copy(
                    src_ref=res.at[slot, src_rows, cols],
                    dst_ref=dland.at[k, dst_rows, cols],
                    send_sem=dsend.at[slot],
                    recv_sem=drecv.at[k],
                    device_id={'dp': partner},
                    device_id_type=pl.DeviceIdType.MESH,
                ).start()

            @pl.when(jnp.logical_and(cond, v < far))
            def _():
                give(pl.ds(pl.multiple_of((1 - c) * hrows, 8), hrows), pl.ds(0, hrows))

            @pl.when(jnp.logical_and(cond, jnp.logical_and(v >= far, core != c)))
            def _():
                give(pl.ds(0, rows), pl.ds(0, rows))

        ks = ks + jnp.where(gives, 1, 0)

        @pl.when(g > 0)
        def _():
            after(pv, ps, 1 - slot, kt, kr)

        takes = jnp.logical_and(g > 0, jnp.logical_or(pv < far, dest(pv)[1] == c))
        kr = kr + jnp.where(takes, 1, 0)
        kt = kt + jnp.where(jnp.logical_and(g > 0, jnp.logical_and(pv < far, ps > 0)), 1, 0)
        return nv, ni, v, i, kt, ks, kr

    zero = jnp.int32(0)
    _, _, pv, pi, kt, ks, kr = lax.fori_loop(0, total, step, (zero,) * 7)
    ps = strip_at(pv, pi)
    before(pv, ps)
    after(pv, ps, (total - 1) % 2, kt, kr)

    for ring in range(RING):
        pltpu.make_async_copy(sbuf.at[ring], sbuf.at[ring], ssend.at[ring]).wait()
    for v in range(far):
        p, _ = dest(jnp.int32(v))
        for width, cond in widths(p, jnp.int32(0))[1:]:
            @pl.when(cond)
            def _():
                block = srem.at[v, :, pl.ds(0, width)]
                pltpu.make_async_copy(block, block, rsend.at[v]).wait()
    pltpu.make_async_copy(fin, fin, fin_sem).wait()


def solution(mesh):
    groups = mesh.shape['dp']

    def local_gram(a_local):
        n_rows, cols = a_local.shape
        rows = n_rows // groups
        hrows = rows // 2
        slots = groups // 2 + 1
        landing = 8 * (slots + 1)
        out, _ = pl.pallas_call(
            functools.partial(kernel, groups),
            out_shape=(
                jax.ShapeDtypeStruct((slots, rows, rows), jnp.float32),
                jax.ShapeDtypeStruct((landing, hrows, MAIN), jnp.float32),
            ),
            in_specs=[pl.BlockSpec(memory_space=pl.ANY)],
            out_specs=(pl.BlockSpec(memory_space=pl.ANY), pl.BlockSpec(memory_space=pl.ANY)),
            scratch_shapes=[
                pltpu.VMEM((2, rows, cols), jnp.bfloat16),
                pltpu.VMEM((2, MAIN, cols), jnp.bfloat16),
                pltpu.VMEM((2, rows, MAIN), jnp.float32),
                pltpu.VMEM((DLAND, rows, MAIN), jnp.float32),
                pltpu.VMEM((RING, hrows, MAIN), jnp.float32),
                pltpu.VMEM((groups - 2, hrows, 384), jnp.float32),
                pltpu.VMEM((2, rows, MAIN), jnp.float32),
                pltpu.VMEM((rows, 384), jnp.float32),
                pltpu.VMEM((rows, rows), jnp.float32),
                pltpu.SemaphoreType.DMA((2,)),
                pltpu.SemaphoreType.DMA((2,)),
                pltpu.SemaphoreType.DMA((2,)),
                pltpu.SemaphoreType.DMA((DLAND,)),
                pltpu.SemaphoreType.REGULAR((DLAND,)),
                pltpu.SemaphoreType.DMA((RING,)),
                pltpu.SemaphoreType.DMA((groups - 2,)),
                pltpu.SemaphoreType.DMA((landing,)),
                pltpu.SemaphoreType.DMA((4,)),
                pltpu.SemaphoreType.DMA,
            ],
            compiler_params=pltpu.CompilerParams(
                collective_id=0, has_side_effects=True, vmem_limit_bytes=67_000_000
            ),
            name='gram_reduce',
        )(a_local)
        return out.reshape(slots, rows, rows)[None]

    return jax.shard_map(local_gram, mesh=mesh, in_specs=(P('mat', 'dp'),), out_specs=P(('mat', 'dp')), check_vma=False)
```
